32 devices in a mesh: dp: 4 (over z), tensor: 8 (over y, x, core).
Axes of the slice: x: 2, y: 2, z: 4, core: 2. Of those that a mesh axis runs over, the one named last changes fastest.
Arguments:
- grad_codes: bfloat16 [8, 1024, 14, 1024], P(None, 'tensor', None, 'dp'), may hold values from -6 to 6
- grad_scales: bfloat16 [8, 1024, 14, 8], P(None, 'tensor', None, 'dp'), may hold values from 0.0099487305 to 0.19921875
- block_slot: int32 [112], replicated, may hold values from 0 to 126, as said below
- left_basis: bfloat16 [128, 1024, 1024], P(('dp', 'tensor')), may hold values from -0.1875 to 0.1875
- right_basis: bfloat16 [128, 1024, 1024], P(('dp', 'tensor')), may hold values from -0.1875 to 0.1875
- first_moment: bfloat16 [128, 1024, 1024], P(('dp', 'tensor')), may hold values from -0.119628906 to 0.119628906
- second_moment: bfloat16 [128, 1024, 1024], P(('dp', 'tensor')), may hold values from 9.9658966e-05 to 0.0099487305
- left_gram: bfloat16 [128, 1024, 1024], P(('dp', 'tensor')), may hold values from -0.59765625 to 0.59765625
- right_gram: bfloat16 [128, 1024, 1024], P(('dp', 'tensor')), may hold values from -0.59765625 to 0.59765625
Outputs:
- update: bfloat16 [8, 1024, 14, 1024], P(None, 'tensor', None, 'dp')
- first_moment_new: bfloat16 [128, 1024, 1024], P(('dp', 'tensor'))
- second_moment_new: bfloat16 [128, 1024, 1024], P(('dp', 'tensor'))
- left_gram_new: bfloat16 [128, 1024, 1024], P(('dp', 'tensor'))
- right_gram_new: bfloat16 [128, 1024, 1024], P(('dp', 'tensor'))
The draws below stay inside these ranges and needn't reach their ends.
Inputs may be any that keep to these rules, and one draw needn't show every extreme that they name: `block_slot`: entries are distinct. Blocks are taken in an order drawn from the seed; the i-th goes to owner i mod 32, in its local slot i div 32, that is global slot (i mod 32) * 4 + i div 32.
All inputs are finite; a program needn't handle non-finite values.
Results may differ from the reference program's by a relative error of at most 0.0065.
Values may be sent and summed in bfloat16 or wider, within the bound.
No kernel may reach another device: no remote copies, remote signals or barrier semaphores. Data moves between devices by JAX's collectives and lax.ppermute only.
A program may use at most 192 MiB of HBM per device.

```python
import math
import jax
import jax.numpy as jnp
from jax import lax

BS = 1024
GROUP = 128
NBR = 8
NBC = 14
NBLK = 112
OWNERS = 32
SLOTS = 4


def draw_block_slot(key, part):
    order = jax.random.permutation(jax.random.fold_in(key, 7), NBLK)
    position = jnp.arange(NBLK, dtype=jnp.int32)
    target = position % OWNERS * SLOTS + position // OWNERS
    return jnp.zeros((NBLK,), jnp.int32).at[order].set(target.astype(jnp.int32))


def steps_of(own_key, extent, split, least, high):
    loudness = 1.0
    for axis_at, blocks in split:
        heights = jax.random.uniform(jax.random.fold_in(jax.random.fold_in(own_key, 6), axis_at), (blocks,), jnp.float32, least / len(split), high / len(split))
        loudness = loudness * jnp.repeat(jnp.exp(heights), extent[axis_at] // blocks).reshape((-1,) + (1,) * (len(extent) - 1 - axis_at))
    return loudness


def bell_draw(stream_key, shape, scale, bound, cuts=(), kind=jnp.bfloat16):
    result = jax.random.normal(stream_key, shape, jnp.float32) * scale
    if len(cuts) > 0:
        result = steps_of(stream_key, shape, cuts, -0.22, 0.18) * result
    return jnp.clip(result, min=-bound, max=bound).astype(kind)


def setup_inputs(seed: int = 0) -> dict:
    arg_keys = jax.random.split(jax.random.key(seed), 10)
    grad_codes = bell_draw(arg_keys[0], (NBR, BS, NBC, BS), 1.0, 6.0, ((1, 8), (3, 4)))
    grad_scales = jnp.clip(jnp.exp(math.log(0.19921875) - 2.9969585 * jax.random.uniform(arg_keys[1], (NBR, BS, NBC, BS // GROUP), jnp.float32) ** steps_of(arg_keys[1], (NBR, BS, NBC, BS // GROUP), ((1, 8), (3, 4)), -0.2, 0.2)), 0.0099487305, 0.19921875).astype(jnp.bfloat16)
    block_slot = draw_block_slot(jax.random.fold_in(arg_keys[9], 71), 0)
    left_basis = bell_draw(arg_keys[3], (OWNERS * SLOTS, BS, BS), BS ** -0.5, 0.1875, ((0, 32),))
    right_basis = bell_draw(arg_keys[4], (OWNERS * SLOTS, BS, BS), BS ** -0.5, 0.1875, ((0, 32),))
    first_moment = bell_draw(arg_keys[5], (OWNERS * SLOTS, BS, BS), 0.02, 0.119628906, ((0, 32),))
    second_moment = jnp.clip(jnp.exp(math.log(0.0099487305) - 4.603446 * jax.random.uniform(arg_keys[6], (OWNERS * SLOTS, BS, BS), jnp.float32) ** steps_of(arg_keys[6], (OWNERS * SLOTS, BS, BS), ((0, 32),), -0.2, 0.2)), 9.965896606445312e-05, 0.0099487305).astype(jnp.bfloat16)
    left_gram = bell_draw(arg_keys[7], (OWNERS * SLOTS, BS, BS), 0.1, 0.59765625, ((0, 32),))
    right_gram = bell_draw(arg_keys[8], (OWNERS * SLOTS, BS, BS), 0.1, 0.59765625, ((0, 32),))
    return dict(grad_codes=grad_codes, grad_scales=grad_scales, block_slot=block_slot, left_basis=left_basis, right_basis=right_basis, first_moment=first_moment, second_moment=second_moment, left_gram=left_gram, right_gram=right_gram)


beta_first = 0.9
beta_second = 0.95
gram_decay = 0.9
epsilon = 1e-08

def soap_block(gradient, left_basis, right_basis, first_moment, second_moment, left_gram, right_gram):
    half = jnp.dot(left_basis.T, gradient, preferred_element_type=jnp.float32).astype(jnp.bfloat16)
    rotated = jnp.dot(half, right_basis, preferred_element_type=jnp.float32)
    moment_one = beta_first * first_moment.astype(jnp.float32) + (1.0 - beta_first) * rotated
    moment_two = beta_second * second_moment.astype(jnp.float32) + (1.0 - beta_second) * rotated * rotated
    direction = (moment_one / (jnp.sqrt(moment_two) + epsilon)).astype(jnp.bfloat16)
    half_back = jnp.dot(left_basis, direction, preferred_element_type=jnp.float32).astype(jnp.bfloat16)
    back = jnp.dot(half_back, right_basis.T, preferred_element_type=jnp.float32)
    left_new = gram_decay * left_gram.astype(jnp.float32) + (1.0 - gram_decay) * jnp.dot(gradient, gradient.T, preferred_element_type=jnp.float32)
    right_new = gram_decay * right_gram.astype(jnp.float32) + (1.0 - gram_decay) * jnp.dot(gradient.T, gradient, preferred_element_type=jnp.float32)
    return (back.astype(jnp.bfloat16), moment_one.astype(jnp.bfloat16), moment_two.astype(jnp.bfloat16), left_new.astype(jnp.bfloat16), right_new.astype(jnp.bfloat16))

def reference(grad_codes, grad_scales, block_slot, left_basis, right_basis, first_moment, second_moment, left_gram, right_gram):
    grouped = grad_codes.astype(jnp.float32).reshape(NBR, BS, NBC, BS // GROUP, GROUP)
    values = (grouped * grad_scales.astype(jnp.float32)[..., None]).reshape(NBR, BS, NBC, BS)
    blocks = values.transpose(0, 2, 1, 3).reshape(NBLK, BS, BS)
    slot_total = OWNERS * SLOTS
    holder = jnp.zeros((slot_total,), jnp.int32).at[block_slot].set(jnp.arange(NBLK, dtype=jnp.int32) + 1)

    def one_slot(position):
        block_index = holder[position]
        present = (block_index > 0).astype(jnp.float32)
        gradient = (blocks[jnp.maximum(block_index - 1, 0)] * present).astype(jnp.bfloat16)
        return soap_block(gradient, left_basis[position], right_basis[position], first_moment[position], second_moment[position], left_gram[position], right_gram[position])
    back, moment_one, moment_two, left_new, right_new = lax.map(one_slot, jnp.arange(slot_total, dtype=jnp.int32))
    placed = back[block_slot].reshape(NBR, NBC, BS, BS).transpose(0, 2, 1, 3)
    return (placed, moment_one, moment_two, left_new, right_new)
```

```python
import functools

import jax
import jax.numpy as jnp
from jax import lax
from jax.experimental import pallas as pl
from jax.experimental.pallas import tpu as pltpu
from jax.sharding import PartitionSpec as P

beta_first = 0.9
beta_second = 0.95
gram_decay = 0.9
epsilon = 1e-08


AXES = ("dp", "tensor")
HBM = pl.BlockSpec(memory_space=pltpu.HBM)
SMEM = pl.BlockSpec(memory_space=pltpu.SMEM)
VMEM = pl.BlockSpec(memory_space=pltpu.VMEM)


def dot(left, right, left_dim=1, right_dim=0):
    return lax.dot_general(
        left,
        right,
        (((left_dim,), (right_dim,)), ((), ())),
        preferred_element_type=jnp.float32,
    )


def fill_holder(block_slot, holder):
    def clear(slot, carry):
        holder[slot] = -1
        return carry

    def put(block, carry):
        holder[block_slot[block]] = block
        return carry

    lax.fori_loop(0, holder.shape[0], clear, 0, unroll=8)
    lax.fori_loop(0, block_slot.shape[0], put, 0, unroll=8)


def pick_kernel(slots, slot_count, counts, packed, block_slot, scales, codes, *rest):
    outs = rest[: 1 if packed else len(slots)]
    holder, tiles, table, sems = rest[len(outs) :]
    fill_holder(block_slot, holder)
    groups, rows = scales.shape[1:]
    cols = codes.shape[2]
    entries = table.shape[0]
    entry = lax.broadcasted_iota(jnp.int32, (entries, cols), 0)
    group = lax.broadcasted_iota(jnp.int32, (entries, cols), 1) // (cols // groups)
    wanted = entry - group

    def tile_copy(index, slot, owner):
        block = holder[owner * slot_count + slot]
        return block, pltpu.make_async_copy(
            codes.at[jnp.maximum(block, 0)], tiles.at[index, owner], sems.at[index, owner]
        )

    for index, slot in enumerate(slots):

        def fetch(owner, carry):
            tile_copy(index, slot, owner)[1].start()
            return carry

        lax.fori_loop(0, counts[index], fetch, 0, unroll=8)

    for index, slot in enumerate(slots):

        def gather(owner, carry):
            block = jnp.maximum(holder[owner * slot_count + slot], 0)
            table[pl.ds(owner * groups, groups), :] = scales[block].astype(jnp.float32)
            return carry

        lax.fori_loop(0, counts[index], gather, 0, unroll=8)
        columns = table[...].T.astype(jnp.bfloat16)

        def scale(owner, carry):
            block, copy = tile_copy(index, slot, owner)
            copy.wait()
            spread = (wanted == owner * groups).astype(jnp.bfloat16)
            wide = dot(columns, spread)
            value = (tiles[index, owner].astype(jnp.float32) * wide).astype(jnp.bfloat16)
            value = jnp.where(block >= 0, value, jnp.zeros_like(value))
            if packed:
                outs[0][owner, index] = value
            else:
                outs[index][owner] = value
            return carry

        lax.fori_loop(0, counts[index], scale, 0, unroll=8)


def pick(slots, counts, packed, slot_count, owners, block_slot, scales, codes):
    rows, cols = codes.shape[1:]
    if packed:
        shapes = [jax.ShapeDtypeStruct((owners, len(slots), rows, cols), jnp.bfloat16)]
    else:
        shapes = [jax.ShapeDtypeStruct((owners, rows, cols), jnp.bfloat16)] * len(slots)
    return pl.pallas_call(
        functools.partial(pick_kernel, slots, slot_count, counts, packed),
        out_shape=shapes,
        in_specs=[SMEM, VMEM, HBM],
        out_specs=[VMEM] * len(shapes),
        scratch_shapes=[
            pltpu.SMEM((owners * slot_count,), jnp.int32),
            pltpu.VMEM((len(slots), owners, rows, cols), jnp.bfloat16),
            pltpu.VMEM((owners * scales.shape[1], rows), jnp.float32),
            pltpu.SemaphoreType.DMA((len(slots), owners)),
        ],
        name="pick",
        cost_estimate=pl.CostEstimate(
            flops=len(slots) * 4000000000, bytes_accessed=4 * owners * rows * cols, transcendentals=0
        ),
    )(block_slot, scales, codes)


def tile_of(owner, stripes, rows):
    return owner // stripes, pl.ds(owner % stripes * rows, rows)


def gradient_copies(received, position, grad, grad_panels, sems):
    owners, _, rows, width = received.shape
    stripes = grad.shape[0] // rows
    copies = []
    for owner in range(owners):
        column, at = tile_of(owner, stripes, rows)
        source = received.at[owner, position]
        whole = grad.at[at, pl.ds(column * width, width)]
        copies.append(pltpu.make_async_copy(source, whole, sems.at[0, owner]))
        if grad_panels is not None:
            copies.append(
                pltpu.make_async_copy(source, grad_panels.at[column, at], sems.at[1, owner])
            )
    return copies


def start_gradient(received, position, limit, me, grad, grad_panels, sems):
    def start():
        for copy in gradient_copies(received, position, grad, grad_panels, sems):
            copy.start()

    if limit is None:
        return start()
    pl.when(me[0] < limit)(start)

    @pl.when(me[0] >= limit)
    def _():
        grad[...] = jnp.zeros(grad.shape, jnp.bfloat16)
        if grad_panels is not None:
            grad_panels[...] = jnp.zeros(grad_panels.shape, jnp.bfloat16)


def wait_gradient(received, position, limit, me, grad, grad_panels, sems):
    def wait():
        for copy in gradient_copies(received, position, grad, grad_panels, sems):
            copy.wait()

    if limit is None:
        return wait()
    pl.when(me[0] < limit)(wait)


def chain_kernel(slot, limit, place_in, sends, chained, me, received, *refs):
    lefts, rights, firsts, seconds = refs[:4]
    refs = refs[4 + chained :]
    send_refs, refs = refs[: len(sends)], refs[len(sends) :]
    first_out, second_out = refs[:2]
    grad, left, left_panels, right, first, second, direction, back, sems, out_sems = refs[2:]
    panels, side, width = back.shape
    rows_of_tile = received.shape[2]
    gradient = (received, place_in, limit, me, grad, None, sems)
    basis = [
        pltpu.make_async_copy(
            lefts.at[slot, :, pl.ds(index * width, width)],
            left_panels.at[index],
            out_sems.at[2, index],
        )
        for index in range(panels)
    ]
    rest = [
        pltpu.make_async_copy(source.at[slot], target, out_sems.at[0, index])
        for index, (source, target) in enumerate(
            ((rights, right), (firsts, first), (seconds, second), (lefts, left))
        )
    ]
    start_gradient(*gradient)
    for copy in basis + rest:
        copy.start()
    wait_gradient(*gradient)
    for copy in basis + rest[:3]:
        copy.wait()

    def rotate(index, carry):
        rows = pl.ds(pl.multiple_of(index * width, width), width)
        half = dot(left_panels[index].T, grad[...]).astype(jnp.bfloat16)
        rotated = dot(half, right[...])
        moment_one = beta_first * first[rows, :].astype(jnp.float32) + (1.0 - beta_first) * rotated
        moment_two = (
            beta_second * second[rows, :].astype(jnp.float32)
            + (1.0 - beta_second) * rotated * rotated
        )
        first[rows, :] = moment_one.astype(jnp.bfloat16)
        second[rows, :] = moment_two.astype(jnp.bfloat16)
        direction[rows, :] = (moment_one / (jnp.sqrt(moment_two) + epsilon)).astype(jnp.bfloat16)
        return carry

    lax.fori_loop(0, panels, rotate, 0)
    moments_out = [
        pltpu.make_async_copy(first, first_out.at[slot], out_sems.at[1, 0]),
        pltpu.make_async_copy(second, second_out.at[slot], out_sems.at[1, 1]),
    ]
    for copy in moments_out:
        copy.start()
    rest[3].wait()

    def rotate_back(index, carry):
        rows = pl.ds(pl.multiple_of(index * width, width), width)
        half_back = dot(left[rows, :], direction[...]).astype(jnp.bfloat16)
        whole = dot(half_back, right[...], 1, 1).astype(jnp.bfloat16)
        for column in range(panels):
            back[column, rows, :] = whole[:, column * width : (column + 1) * width]
        return carry

    lax.fori_loop(0, panels, rotate_back, 0)
    sends_out = []
    for index, (low, high, position) in enumerate(sends):
        for owner in range(low, high):
            column, rows = tile_of(owner, side // rows_of_tile, rows_of_tile)
            sends_out.append(
                pltpu.make_async_copy(
                    back.at[column, rows], send_refs[index].at[owner, position], sems.at[0, owner]
                )
            )
    for copy in sends_out:
        copy.start()
    for copy in moments_out + sends_out:
        copy.wait()


def chain_step(slot, limit, place_in, sends, widths, targets, state, me, received, arrays):
    owners, _, rows, width = received.shape
    side = arrays[0].shape[1]
    panels = side // width
    square = pltpu.VMEM((side, side), jnp.bfloat16)
    columns = pltpu.VMEM((panels, side, width), jnp.bfloat16)
    aliased, aliases = [], {}
    for index, target in enumerate(list(targets) + list(state)):
        if target is not None:
            aliases[6 + len(aliased)] = index
            aliased.append(target)
    moved = [
        jax.ShapeDtypeStruct((owners, count, rows, width), jnp.bfloat16) for count in widths
    ]
    kept = jax.ShapeDtypeStruct(arrays[0].shape, jnp.bfloat16)
    results = pl.pallas_call(
        functools.partial(chain_kernel, slot, limit, place_in, sends, len(aliased)),
        out_shape=moved + [kept] * 2,
        in_specs=[SMEM] + [HBM] * (5 + len(aliased)),
        out_specs=[HBM] * (len(sends) + 2),
        scratch_shapes=[
            square,
            square,
            columns,
            square,
            square,
            square,
            square,
            columns,
            pltpu.SemaphoreType.DMA((1, owners)),
            pltpu.SemaphoreType.DMA((3, max(4, panels))),
        ],
        input_output_aliases=aliases,
        name="chain",
        cost_estimate=pl.CostEstimate(
            flops=8 * side**3, bytes_accessed=16 * side * side, transcendentals=side * side
        ),
    )(me, received, *arrays[:4], *aliased)
    return results[: len(sends)], results[len(sends) :]


def gram_kernel(slot, limit, place_in, extra, me, received, left_grams, right_grams, *refs):
    left_out, right_out, grad, grad_panels, left_gram, right_gram, sems, out_sems = refs[extra:]
    panels, side, width = grad_panels.shape
    gradient = (received, place_in, limit, me, grad, grad_panels, sems)
    loads = [
        pltpu.make_async_copy(left_grams.at[slot], left_gram, out_sems.at[0]),
        pltpu.make_async_copy(right_grams.at[slot], right_gram, out_sems.at[1]),
    ]
    start_gradient(*gradient)
    for copy in loads:
        copy.start()
    wait_gradient(*gradient)
    for copy in loads:
        copy.wait()

    def grams(index, carry):
        rows = pl.ds(pl.multiple_of(index * width, width), width)
        left_new = gram_decay * left_gram[rows, :].astype(jnp.float32) + (
            1.0 - gram_decay
        ) * dot(grad[rows, :], grad[...], 1, 1)
        left_gram[rows, :] = left_new.astype(jnp.bfloat16)
        right_new = gram_decay * right_gram[rows, :].astype(jnp.float32) + (
            1.0 - gram_decay
        ) * dot(grad_panels[index].T, grad[...])
        right_gram[rows, :] = right_new.astype(jnp.bfloat16)
        return carry

    lax.fori_loop(0, panels, grams, 0)
    stores = [
        pltpu.make_async_copy(left_gram, left_out.at[slot], out_sems.at[0]),
        pltpu.make_async_copy(right_gram, right_out.at[slot], out_sems.at[1]),
    ]
    for copy in stores:
        copy.start()
    for copy in stores:
        copy.wait()


def gram_step(slot, limit, place_in, state, after, me, received, arrays):
    owners, _, _, width = received.shape
    side = arrays[0].shape[1]
    panels = side // width
    square = pltpu.VMEM((side, side), jnp.bfloat16)
    aliased = [array for array in state if array is not None]
    kept = jax.ShapeDtypeStruct(arrays[0].shape, jnp.bfloat16)
    extra = len(aliased) + len(after)
    return pl.pallas_call(
        functools.partial(gram_kernel, slot, limit, place_in, extra),
        out_shape=[kept] * 2,
        in_specs=[SMEM] + [HBM] * (3 + extra),
        out_specs=[HBM] * 2,
        scratch_shapes=[
            square,
            pltpu.VMEM((panels, side, width), jnp.bfloat16),
            square,
            square,
            pltpu.SemaphoreType.DMA((2, owners)),
            pltpu.SemaphoreType.DMA((2,)),
        ],
        input_output_aliases={4 + index: index for index in range(len(aliased))},
        name="gram",
        cost_estimate=pl.CostEstimate(
            flops=4 * side**3, bytes_accessed=12 * side * side, transcendentals=0
        ),
    )(me, received, *arrays[4:], *aliased, *after)


def place_kernel(jobs, slot_count, total, chained, me, block_slot, *refs):
    sources = refs[:total]
    out, holder = refs[total + chained : total + chained + 2]
    tiles, sems, out_sems = refs[total + chained + 2 :]
    fill_holder(block_slot, holder)

    def each(stage):
        start = 0
        for source, position, slot, count, low, high in jobs:

            def move(here, owner, taken):
                block = holder[owner * slot_count + slot]

                def arrive():
                    return pltpu.make_async_copy(taken, tiles.at[here], sems.at[here])

                def leave():
                    held = taken if position is None else tiles.at[here]
                    return pltpu.make_async_copy(held, out.at[block], out_sems.at[here])

                @pl.when(block >= 0)
                def _():
                    if position is None:
                        if stage == 0:
                            leave().start()
                        elif stage == 2:
                            leave().wait()
                    elif stage == 0:
                        arrive().start()
                    elif stage == 1:
                        arrive().wait()
                        leave().start()
                    else:
                        leave().wait()

            def act(owner, carry, source=source, position=position, move=move, start=start):
                move(start + owner, owner, sources[source].at[owner, position])
                return carry

            @pl.when(jnp.logical_and(me[0] >= low, me[0] < high))
            def _():
                if position is None:
                    for shift in range(count):
                        move(start + shift, me[0] ^ shift, sources[source + shift])
                else:
                    lax.fori_loop(0, count, act, 0)

            start += count

    for stage in range(3):
        each(stage)


def place(jobs, slot_count, owners, update, shape, me, block_slot, sources):
    chained = 0 if update is None else 1
    total = sum(job[3] for job in jobs)
    specs = [VMEM if source.ndim == 2 else HBM for source in sources]
    return pl.pallas_call(
        functools.partial(place_kernel, jobs, slot_count, len(sources), chained),
        out_shape=jax.ShapeDtypeStruct(shape, jnp.bfloat16),
        in_specs=[SMEM, SMEM] + specs + [HBM] * chained,
        out_specs=HBM,
        scratch_shapes=[
            pltpu.SMEM((owners * slot_count,), jnp.int32),
            pltpu.VMEM((total,) + shape[1:], jnp.bfloat16),
            pltpu.SemaphoreType.DMA((total,)),
            pltpu.SemaphoreType.DMA((total,)),
        ],
        input_output_aliases={2 + len(sources): 0} if chained else {},
        name="place",
        cost_estimate=pl.CostEstimate(
            flops=1000000000,
            bytes_accessed=4 * total * shape[1] * shape[2],
            transcendentals=0,
        ),
    )(me, block_slot, *sources, *([update] if chained else []))


def exchange(tiles):
    return lax.all_to_all(tiles, AXES, split_axis=0, concat_axis=0, tiled=True)


def on_device(grad_codes, grad_scales, block_slot, *arrays):
    dp_count = lax.axis_size("dp")
    tensor_count = lax.axis_size("tensor")
    owners = dp_count * tensor_count
    slot_count = arrays[0].shape[0]
    block_rows, tile_rows, block_cols, tile_cols = grad_codes.shape
    blocks = block_rows * block_cols
    me = (lax.axis_index("dp") * tensor_count + lax.axis_index("tensor")).astype(jnp.int32)
    me = me.reshape(1)
    codes = grad_codes.transpose(0, 2, 1, 3).reshape(blocks, tile_rows, tile_cols)
    scales = grad_scales.transpose(0, 2, 3, 1).reshape(blocks, -1, tile_rows)
    shape = (blocks, tile_rows, tile_cols)
    half = owners // 2
    merged = slot_count > 2 and owners % 2 == 0 and blocks == owners * (slot_count - 1) + half

    def take(slots, counts, packed):
        return pick(slots, counts, packed, slot_count, owners, block_slot, scales, codes)

    def chain(slot, received, place_in, state, sends, widths, targets, limit=None):
        return chain_step(
            slot, limit, place_in, sends, widths, targets, state, me, received, arrays
        )

    def gram(slot, received, place_in, state, after, limit=None):
        return gram_step(slot, limit, place_in, state, after, me, received, arrays)

    def put(jobs, update, sources):
        return place(tuple(jobs), slot_count, owners, update, shape, me, block_slot, sources)

    moments, grams, update = (None, None), (None, None), None
    if not merged:
        received = [exchange(take((slot,), (owners,), True)[0]) for slot in range(slot_count)]
        for slot in range(slot_count):
            (sent,), moments = chain(
                slot, received[slot], 0, moments, ((0, owners, 0),), (1,), (None,)
            )
            grams = gram(slot, received[slot], 0, grams, ())
            update = put([(0, 0, slot, owners, 0, owners)], update, (exchange(sent),))
    else:
        last = slot_count - 1
        middle = tuple(range(1, last))
        low, high = (0, half, 0), (half, owners, 0)
        first = exchange(take((0,), (owners,), True)[0])
        bulk = exchange(take(middle, (owners,) * len(middle), True)[0])
        early = take((last,), (half,), True)[0]
        (early, late), moments = chain(0, first, 0, moments, (high, low), (1, 1), (early, None))
        grams = gram(0, first, 0, grams, ())
        early, *grams = lax.optimization_barrier((early, *grams))
        early = exchange(early)
        sent = None
        for index, slot in enumerate(middle):
            (sent,), moments = chain(
                slot, bulk, index, moments, ((0, owners, index),), (len(middle),), (sent,)
            )
        returned = exchange(sent)
        (late, near), moments = chain(
            last, early, 0, moments, (high, low), (1, 1), (late, None), half
        )
        near = near.reshape(owners, tile_rows, tile_cols)
        pieces = []
        for shift in range(half):
            piece = lax.dynamic_index_in_dim(near, me[0] ^ shift, 0, keepdims=False)
            if shift:
                piece = lax.ppermute(piece, AXES, [(at, at ^ shift) for at in range(half)])
            pieces.append(piece)
        grams = gram(middle[0], bulk, 0, grams, (early,))
        late, *rest = lax.optimization_barrier((late, *grams, *pieces))
        grams, pieces = rest[:2], rest[2:]
        late = exchange(late)
        for index, slot in enumerate(middle[1:], 1):
            grams = gram(slot, bulk, index, grams, (returned,))
        grams = gram(last, early, 0, grams, (returned,), half)
        jobs = [(0, index, slot, owners, 0, owners) for index, slot in enumerate(middle)]
        jobs.append((1, 0, 0, owners, half, owners))
        jobs.append((2, None, last, half, 0, half))
        update = put(jobs, update, (returned, early, *pieces))
        jobs = ((0, 0, 0, owners, 0, half), (0, 0, last, half, half, owners))
        update = put(jobs, update, (late,))
    state = (*moments, *grams)
    update = update.reshape(block_rows, block_cols, tile_rows, tile_cols).transpose(0, 2, 1, 3)
    return (update, *state)


def solution(mesh):
    tiled = P(None, "tensor", None, "dp")
    owned = P(AXES, None, None)
    return jax.shard_map(
        on_device,
        mesh=mesh,
        in_specs=(tiled, tiled, P()) + (owned,) * 6,
        out_specs=(tiled,) + (owned,) * 4,
        check_vma=False,
    )
```

```python
import functools

import jax
import jax.numpy as jnp
from jax import lax
from jax.experimental import pallas as pl
from jax.experimental.pallas import tpu as pltpu
from jax.sharding import PartitionSpec as P


beta_first = 0.9
beta_second = 0.95
gram_decay = 0.9
epsilon = 1e-08


AXES = ("dp", "tensor")
HBM = pl.BlockSpec(memory_space=pltpu.HBM)
SMEM = pl.BlockSpec(memory_space=pltpu.SMEM)
VMEM = pl.BlockSpec(memory_space=pltpu.VMEM)


def dot(left, right, left_dim=1, right_dim=0):
    return lax.dot_general(
        left,
        right,
        (((left_dim,), (right_dim,)), ((), ())),
        preferred_element_type=jnp.float32,
    )


def fill_holder(block_slot, holder):
    def clear(slot, carry):
        holder[slot] = -1
        return carry

    def put(block, carry):
        holder[block_slot[block]] = block
        return carry

    lax.fori_loop(0, holder.shape[0], clear, 0, unroll=8)
    lax.fori_loop(0, block_slot.shape[0], put, 0, unroll=8)


def pick_kernel(slots, slot_count, counts, folded, extra, me, block_slot, scales, codes, *rest):
    *outs, holder, tiles, table, sems = rest[extra:]
    fill_holder(block_slot, holder)
    groups, _ = scales.shape[1:]
    cols = codes.shape[2]
    span = cols // groups
    step = 8

    def owner_at(position):
        return me[0] ^ position if folded else position

    def tile_copy(index, slot, owner):
        block = holder[owner_at(owner) * slot_count + slot]
        return block, pltpu.make_async_copy(
            codes.at[jnp.maximum(block, 0)], tiles.at[index, owner], sems.at[index, owner]
        )

    for index, slot in enumerate(slots):

        def fetch(owner, carry):
            tile_copy(index, slot, owner)[1].start()
            return carry

        lax.fori_loop(0, counts[index], fetch, 0, unroll=8)

    for index, slot in enumerate(slots):

        def gather(owner, carry):
            block = jnp.maximum(holder[owner_at(owner) * slot_count + slot], 0)
            table[pl.ds(owner * groups, groups), :] = scales[block].astype(jnp.float32)
            return carry

        lax.fori_loop(0, counts[index], gather, 0, unroll=8)
        columns = table[...].T
        for start in range(0, counts[index], step):
            owners = range(start, min(start + step, counts[index]))
            held = []
            for owner in owners:
                block, copy = tile_copy(index, slot, owner)
                copy.wait()
                held.append(block)
            for owner, block in zip(owners, held):
                for group in range(groups):
                    at = owner * groups + group
                    lanes = slice(group * span, (group + 1) * span)
                    value = tiles[index, owner, :, lanes].astype(jnp.float32)
                    value = (value * columns[:, at : at + 1]).astype(jnp.bfloat16)
                    value = jnp.where(block >= 0, value, jnp.zeros_like(value))
                    if folded:
                        outs[owner // folded][owner % folded, :, lanes] = value
                    else:
                        outs[0][owner, index, :, lanes] = value


def pick(slots, counts, folded, after, slot_count, owners, me, block_slot, scales, codes):
    rows, cols = codes.shape[1:]
    if folded:
        shapes = [jax.ShapeDtypeStruct((folded, rows, cols), jnp.bfloat16)] * (owners // folded)
    else:
        shapes = [jax.ShapeDtypeStruct((owners, len(slots), rows, cols), jnp.bfloat16)]
    return pl.pallas_call(
        functools.partial(pick_kernel, slots, slot_count, counts, folded, len(after)),
        out_shape=shapes,
        in_specs=[SMEM, SMEM, VMEM, HBM] + [HBM] * len(after),
        out_specs=[VMEM] * len(shapes),
        scratch_shapes=[
            pltpu.SMEM((owners * slot_count,), jnp.int32),
            pltpu.VMEM((len(slots), owners, rows, cols), jnp.bfloat16),
            pltpu.VMEM((owners * scales.shape[1], rows), jnp.float32),
            pltpu.SemaphoreType.DMA((len(slots), owners)),
        ],
        name="pick",
        cost_estimate=pl.CostEstimate(
            flops=len(slots) * 4000000000, bytes_accessed=4 * owners * rows * cols, transcendentals=0
        ),
    )(me, block_slot, scales, codes, *after)


def tile_of(owner, stripes, rows):
    return owner // stripes, pl.ds(owner % stripes * rows, rows)


def gradient_copies(received, position, me, grad, grad_panels, sems):
    rows, width = received[0].shape[-2:]
    stripes = grad.shape[0] // rows
    copies = []
    for index in range(stripes * (grad.shape[1] // width)):
        if position is None:
            source = received[index % stripes].at[index // stripes]
            column, stripe = (me[0] // stripes) ^ (index // stripes), (me[0] % stripes) ^ (
                index % stripes
            )
        else:
            source = received[0].at[index, position]
            column, stripe = index // stripes, index % stripes
        at = pl.ds(pl.multiple_of(stripe * rows, rows), rows)
        whole = grad.at[at, pl.ds(pl.multiple_of(column * width, width), width)]
        copies.append(pltpu.make_async_copy(source, whole, sems.at[0, index]))
        if grad_panels is not None:
            copies.append(
                pltpu.make_async_copy(source, grad_panels.at[column, at], sems.at[1, index])
            )
    return copies


def start_gradient(received, position, limit, me, grad, grad_panels, sems):
    def start():
        for copy in gradient_copies(received, position, me, grad, grad_panels, sems):
            copy.start()

    if limit is None:
        return start()
    pl.when(me[0] < limit)(start)

    @pl.when(me[0] >= limit)
    def _():
        grad[...] = jnp.zeros(grad.shape, jnp.bfloat16)
        if grad_panels is not None:
            grad_panels[...] = jnp.zeros(grad_panels.shape, jnp.bfloat16)


def wait_gradient(received, position, limit, me, grad, grad_panels, sems):
    def wait():
        for copy in gradient_copies(received, position, me, grad, grad_panels, sems):
            copy.wait()

    if limit is None:
        return wait()
    pl.when(me[0] < limit)(wait)


def chain_kernel(slot, limit, parts, place_in, sends, chained, me, *refs):
    received, refs = refs[:parts], refs[parts:]
    lefts, rights, firsts, seconds = refs[:4]
    refs = refs[4 + chained :]
    send_refs, refs = refs[: len(sends)], refs[len(sends) :]
    first_out, second_out = refs[:2]
    grad, left, left_panels, right, first, second, direction, back, sems, out_sems = refs[2:]
    panels, side, width = back.shape
    rows_of_tile = received[0].shape[-2]
    gradient = (received, place_in, limit, me, grad, None, sems)
    basis = [
        pltpu.make_async_copy(
            lefts.at[slot, :, pl.ds(index * width, width)],
            left_panels.at[index],
            out_sems.at[2, index],
        )
        for index in range(panels)
    ]
    rest = [
        pltpu.make_async_copy(source.at[slot], target, out_sems.at[0, index])
        for index, (source, target) in enumerate(
            ((rights, right), (firsts, first), (seconds, second), (lefts, left))
        )
    ]
    start_gradient(*gradient)
    for copy in basis + rest:
        copy.start()
    wait_gradient(*gradient)
    for copy in basis + rest[:3]:
        copy.wait()

    def rotate(index, carry):
        rows = pl.ds(pl.multiple_of(index * width, width), width)
        half = dot(left_panels[index].T, grad[...]).astype(jnp.bfloat16)
        rotated = dot(half, right[...])
        moment_one = beta_first * first[rows, :].astype(jnp.float32) + (1.0 - beta_first) * rotated
        moment_two = (
            beta_second * second[rows, :].astype(jnp.float32)
            + (1.0 - beta_second) * rotated * rotated
        )
        first[rows, :] = moment_one.astype(jnp.bfloat16)
        second[rows, :] = moment_two.astype(jnp.bfloat16)
        direction[rows, :] = (moment_one / (jnp.sqrt(moment_two) + epsilon)).astype(jnp.bfloat16)
        return carry

    lax.fori_loop(0, panels, rotate, 0)
    moments_out = [
        pltpu.make_async_copy(first, first_out.at[slot], out_sems.at[1, 0]),
        pltpu.make_async_copy(second, second_out.at[slot], out_sems.at[1, 1]),
    ]
    for copy in moments_out:
        copy.start()
    rest[3].wait()

    def rotate_back(index, carry):
        rows = pl.ds(pl.multiple_of(index * width, width), width)
        half_back = dot(left[rows, :], direction[...]).astype(jnp.bfloat16)
        whole = dot(half_back, right[...], 1, 1).astype(jnp.bfloat16)
        for column in range(panels):
            back[column, rows, :] = whole[:, column * width : (column + 1) * width]
        return carry

    lax.fori_loop(0, panels, rotate_back, 0)
    sends_out = []
    for index, (low, high, position) in enumerate(sends):
        for owner in range(low, high):
            column, rows = tile_of(owner, side // rows_of_tile, rows_of_tile)
            sends_out.append(
                pltpu.make_async_copy(
                    back.at[column, rows], send_refs[index].at[owner, position], sems.at[0, owner]
                )
            )
    for copy in sends_out:
        copy.start()
    for copy in moments_out + sends_out:
        copy.wait()


def chain_step(slot, limit, place_in, sends, widths, targets, state, me, received, arrays):
    rows, width = received[0].shape[-2:]
    side = arrays[0].shape[1]
    panels = side // width
    owners = panels * (side // rows)
    square = pltpu.VMEM((side, side), jnp.bfloat16)
    columns = pltpu.VMEM((panels, side, width), jnp.bfloat16)
    aliased, aliases = [], {}
    for index, target in enumerate(list(targets) + list(state)):
        if target is not None:
            aliases[5 + len(received) + len(aliased)] = index
            aliased.append(target)
    moved = [
        jax.ShapeDtypeStruct((owners, count, rows, width), jnp.bfloat16) for count in widths
    ]
    kept = jax.ShapeDtypeStruct(arrays[0].shape, jnp.bfloat16)
    results = pl.pallas_call(
        functools.partial(
            chain_kernel, slot, limit, len(received), place_in, sends, len(aliased)
        ),
        out_shape=moved + [kept] * 2,
        in_specs=[SMEM] + [HBM] * (4 + len(received) + len(aliased)),
        out_specs=[HBM] * (len(sends) + 2),
        scratch_shapes=[
            square,
            square,
            columns,
            square,
            square,
            square,
            square,
            columns,
            pltpu.SemaphoreType.DMA((1, owners)),
            pltpu.SemaphoreType.DMA((3, max(4, panels))),
        ],
        input_output_aliases=aliases,
        name="chain",
        cost_estimate=pl.CostEstimate(
            flops=8 * side**3, bytes_accessed=16 * side * side, transcendentals=side * side
        ),
    )(me, *received, *arrays[:4], *aliased)
    return results[: len(sends)], results[len(sends) :]


def gram_kernel(slot, limit, parts, place_in, extra, me, *refs):
    received, (left_grams, right_grams), refs = refs[:parts], refs[parts : parts + 2], refs[parts + 2 :]
    left_out, right_out, grad, grad_panels, left_gram, right_gram, sems, out_sems = refs[extra:]
    panels, _, width = grad_panels.shape
    gradient = (received, place_in, limit, me, grad, grad_panels, sems)
    loads = [
        pltpu.make_async_copy(left_grams.at[slot], left_gram, out_sems.at[0]),
        pltpu.make_async_copy(right_grams.at[slot], right_gram, out_sems.at[1]),
    ]
    start_gradient(*gradient)
    for copy in loads:
        copy.start()
    wait_gradient(*gradient)
    for copy in loads:
        copy.wait()

    def grams(index, carry):
        rows = pl.ds(pl.multiple_of(index * width, width), width)
        left_new = gram_decay * left_gram[rows, :].astype(jnp.float32) + (
            1.0 - gram_decay
        ) * dot(grad[rows, :], grad[...], 1, 1)
        left_gram[rows, :] = left_new.astype(jnp.bfloat16)
        right_new = gram_decay * right_gram[rows, :].astype(jnp.float32) + (
            1.0 - gram_decay
        ) * dot(grad_panels[index].T, grad[...])
        right_gram[rows, :] = right_new.astype(jnp.bfloat16)
        return carry

    lax.fori_loop(0, panels, grams, 0)
    stores = [
        pltpu.make_async_copy(left_gram, left_out.at[slot], out_sems.at[0]),
        pltpu.make_async_copy(right_gram, right_out.at[slot], out_sems.at[1]),
    ]
    for copy in stores:
        copy.start()
    for copy in stores:
        copy.wait()


def gram_step(slot, limit, place_in, state, after, me, received, arrays):
    rows, width = received[0].shape[-2:]
    side = arrays[0].shape[1]
    panels = side // width
    owners = panels * (side // rows)
    square = pltpu.VMEM((side, side), jnp.bfloat16)
    aliased = [array for array in state if array is not None]
    kept = jax.ShapeDtypeStruct(arrays[0].shape, jnp.bfloat16)
    extra = len(aliased) + len(after)
    return pl.pallas_call(
        functools.partial(gram_kernel, slot, limit, len(received), place_in, extra),
        out_shape=[kept] * 2,
        in_specs=[SMEM] + [HBM] * (2 + len(received) + extra),
        out_specs=[HBM] * 2,
        scratch_shapes=[
            square,
            pltpu.VMEM((panels, side, width), jnp.bfloat16),
            square,
            square,
            pltpu.SemaphoreType.DMA((2, owners)),
            pltpu.SemaphoreType.DMA((2,)),
        ],
        input_output_aliases={
            3 + len(received) + index: index for index in range(len(aliased))
        },
        name="gram",
        cost_estimate=pl.CostEstimate(
            flops=4 * side**3, bytes_accessed=12 * side * side, transcendentals=0
        ),
    )(me, *received, *arrays[4:], *aliased, *after)


def place_kernel(jobs, slot_count, total, chained, me, block_slot, *refs):
    sources = refs[:total]
    out, holder = refs[total + chained : total + chained + 2]
    tiles, sems, out_sems = refs[total + chained + 2 :]
    fill_holder(block_slot, holder)

    def each(stage):
        start = 0
        for source, position, slot, count, low, high in jobs:

            def move(here, owner, taken):
                block = holder[owner * slot_count + slot]

                def arrive():
                    return pltpu.make_async_copy(taken, tiles.at[here], sems.at[here])

                def leave():
                    held = taken if position is None else tiles.at[here]
                    return pltpu.make_async_copy(held, out.at[block], out_sems.at[here])

                @pl.when(block >= 0)
                def _():
                    if position is None:
                        if stage == 0:
                            leave().start()
                        elif stage == 2:
                            leave().wait()
                    elif stage == 0:
                        arrive().start()
                    elif stage == 1:
                        arrive().wait()
                        leave().start()
                    else:
                        leave().wait()

            def act(owner, carry, source=source, position=position, move=move, start=start):
                move(start + owner, owner, sources[source].at[owner, position])
                return carry

            @pl.when(jnp.logical_and(me[0] >= low, me[0] < high))
            def _():
                if position is None:
                    for shift in range(count):
                        move(start + shift, me[0] ^ shift, sources[source + shift])
                else:
                    lax.fori_loop(0, count, act, 0)

            start += count

    for stage in range(3):
        each(stage)


def place(jobs, slot_count, owners, update, shape, me, block_slot, sources):
    chained = 0 if update is None else 1
    total = sum(job[3] for job in jobs)
    specs = [VMEM if source.ndim == 2 else HBM for source in sources]
    return pl.pallas_call(
        functools.partial(place_kernel, jobs, slot_count, len(sources), chained),
        out_shape=jax.ShapeDtypeStruct(shape, jnp.bfloat16),
        in_specs=[SMEM, SMEM] + specs + [HBM] * chained,
        out_specs=HBM,
        scratch_shapes=[
            pltpu.SMEM((owners * slot_count,), jnp.int32),
            pltpu.VMEM((total,) + shape[1:], jnp.bfloat16),
            pltpu.SemaphoreType.DMA((total,)),
            pltpu.SemaphoreType.DMA((total,)),
        ],
        input_output_aliases={2 + len(sources): 0} if chained else {},
        name="place",
        cost_estimate=pl.CostEstimate(
            flops=1000000000,
            bytes_accessed=4 * total * shape[1] * shape[2],
            transcendentals=0,
        ),
    )(me, block_slot, *sources, *([update] if chained else []))


def exchange(tiles):
    return lax.all_to_all(tiles, AXES, split_axis=0, concat_axis=0, tiled=True)


def fold(arrays, dp_count, tensor_count):
    moved = [arrays[0]]
    for shift in range(1, dp_count):
        moved.append(
            lax.ppermute(arrays[shift], "dp", [(at, at ^ shift) for at in range(dp_count)])
        )
    given = []
    for shift in range(tensor_count):
        stacked = jnp.stack([array[shift] for array in moved])
        if shift:
            stacked = lax.ppermute(
                stacked, "tensor", [(at, at ^ shift) for at in range(tensor_count)]
            )
        given.append(stacked)
    return given


def on_device(grad_codes, grad_scales, block_slot, *arrays):
    dp_count = lax.axis_size("dp")
    tensor_count = lax.axis_size("tensor")
    owners = dp_count * tensor_count
    slot_count = arrays[0].shape[0]
    block_rows, tile_rows, block_cols, tile_cols = grad_codes.shape
    blocks = block_rows * block_cols
    me = (lax.axis_index("dp") * tensor_count + lax.axis_index("tensor")).astype(jnp.int32)
    me = me.reshape(1)
    codes = grad_codes.transpose(0, 2, 1, 3).reshape(blocks, tile_rows, tile_cols)
    scales = grad_scales.transpose(0, 2, 3, 1).reshape(blocks, -1, tile_rows)
    shape = (blocks, tile_rows, tile_cols)
    half = owners // 2
    merged = (
        slot_count > 2
        and blocks == owners * (slot_count - 1) + half
        and dp_count & (dp_count - 1) == 0
        and tensor_count & (tensor_count - 1) == 0
    )

    def take(slots, counts, folded=None, after=()):
        return pick(
            slots, counts, folded, after, slot_count, owners, me, block_slot, scales, codes
        )

    def chain(slot, received, place_in, state, sends, widths, targets, limit=None):
        return chain_step(
            slot, limit, place_in, sends, widths, targets, state, me, received, arrays
        )

    def gram(slot, received, place_in, state, after, limit=None):
        return gram_step(slot, limit, place_in, state, after, me, received, arrays)

    def put(jobs, update, sources):
        return place(tuple(jobs), slot_count, owners, update, shape, me, block_slot, sources)

    moments, grams, update = (None, None), (None, None), None
    if not merged:
        received = [exchange(take((slot,), (owners,))[0]) for slot in range(slot_count)]
        for slot in range(slot_count):
            (sent,), moments = chain(
                slot, received[slot : slot + 1], 0, moments, ((0, owners, 0),), (1,), (None,)
            )
            grams = gram(slot, received[slot : slot + 1], 0, grams, ())
            update = put([(0, 0, slot, owners, 0, owners)], update, (exchange(sent),))
    else:
        last = slot_count - 1
        middle = tuple(range(1, last))
        low, high = (0, half, 0), (half, owners, 0)
        first = take((0,), (owners,), tensor_count)
        bulk = take(middle, (owners,) * len(middle), None, first[-1:])[0]
        bulk = exchange(bulk)
        first = fold(first, dp_count, tensor_count)
        early = take((last,), (half,))[0]
        (early, late), moments = chain(0, first, None, moments, (high, low), (1, 1), (early, None))
        early = exchange(early)
        sent = None
        for index, slot in enumerate(middle):
            (sent,), moments = chain(
                slot, [bulk], index, moments, ((0, owners, index),), (len(middle),), (sent,)
            )
        returned = exchange(sent)
        (late, near), moments = chain(
            last, [early], 0, moments, (high, low), (1, 1), (late, None), half
        )
        near = near.reshape(owners, tile_rows, tile_cols)
        pieces = []
        for shift in range(half):
            piece = lax.dynamic_index_in_dim(near, me[0] ^ shift, 0, keepdims=False)
            if shift:
                piece = lax.ppermute(piece, AXES, [(at, at ^ shift) for at in range(half)])
            pieces.append(piece)
        grams = gram(0, first, None, grams, (early,))
        late, *rest = lax.optimization_barrier((late, *grams, *pieces))
        grams, pieces = rest[:2], rest[2:]
        late = exchange(late)
        for index, slot in enumerate(middle):
            grams = gram(slot, [bulk], index, grams, (returned,))
        grams = gram(last, [early], 0, grams, (returned,), half)
        jobs = [(0, index, slot, owners, 0, owners) for index, slot in enumerate(middle)]
        jobs.append((1, 0, 0, owners, half, owners))
        jobs.append((2, None, last, half, 0, half))
        update = put(jobs, update, (returned, early, *pieces))
        jobs = ((0, 0, 0, owners, 0, half), (0, 0, last, half, half, owners))
        update = put(jobs, update, (late,))
    state = (*moments, *grams)
    update = update.reshape(block_rows, block_cols, tile_rows, tile_cols).transpose(0, 2, 1, 3)
    return (update, *state)


def solution(mesh):
    tiled = P(None, "tensor", None, "dp")
    owned = P(AXES, None, None)

    return jax.shard_map(
        on_device,
        mesh=mesh,
        in_specs=(tiled, tiled, P()) + (owned,) * 6,
        out_specs=(tiled,) + (owned,) * 4,
        check_vma=False,
    )
```

```python
import functools

import jax
import jax.numpy as jnp
from jax import lax
from jax.experimental import pallas as pl
from jax.experimental.pallas import tpu as pltpu
from jax.sharding import PartitionSpec as P


beta_first = 0.9
beta_second = 0.95
gram_decay = 0.9
epsilon = 1e-08


AXES = ("dp", "tensor")
HBM = pl.BlockSpec(memory_space=pltpu.HBM)
SMEM = pl.BlockSpec(memory_space=pltpu.SMEM)
VMEM = pl.BlockSpec(memory_space=pltpu.VMEM)


def dot(left, right, left_dim=1, right_dim=0):
    return lax.dot_general(
        left,
        right,
        (((left_dim,), (right_dim,)), ((), ())),
        preferred_element_type=jnp.float32,
    )


def fill_holder(block_slot, holder):
    def clear(slot, carry):
        holder[slot] = -1
        return carry

    def put(block, carry):
        holder[block_slot[block]] = block
        return carry

    lax.fori_loop(0, holder.shape[0], clear, 0, unroll=8)
    lax.fori_loop(0, block_slot.shape[0], put, 0, unroll=8)


def pick_kernel(slots, slot_count, counts, folded, extra, me, block_slot, scales, codes, *rest):
    *outs, holder, tiles, table, sems = rest[extra:]
    fill_holder(block_slot, holder)
    groups, _ = scales.shape[1:]
    cols = codes.shape[2]
    span = cols // groups
    step = 8

    def owner_at(position):
        return me[0] ^ position if folded else position

    def tile_copy(index, slot, owner):
        block = holder[owner_at(owner) * slot_count + slot]
        return block, pltpu.make_async_copy(
            codes.at[jnp.maximum(block, 0)], tiles.at[index, owner], sems.at[index, owner]
        )

    for index, slot in enumerate(slots):

        def fetch(owner, carry):
            tile_copy(index, slot, owner)[1].start()
            return carry

        lax.fori_loop(0, counts[index], fetch, 0, unroll=8)

    for index, slot in enumerate(slots):

        def gather(owner, carry):
            block = jnp.maximum(holder[owner_at(owner) * slot_count + slot], 0)
            table[pl.ds(owner * groups, groups), :] = scales[block].astype(jnp.float32)
            return carry

        lax.fori_loop(0, counts[index], gather, 0, unroll=8)
        columns = table[...].T
        for start in range(0, counts[index], step):
            owners = range(start, min(start + step, counts[index]))
            held = []
            for owner in owners:
                block, copy = tile_copy(index, slot, owner)
                copy.wait()
                held.append(block)
            for owner, block in zip(owners, held):
                for group in range(groups):
                    at = owner * groups + group
                    lanes = slice(group * span, (group + 1) * span)
                    value = tiles[index, owner, :, lanes].astype(jnp.float32)
                    value = (value * columns[:, at : at + 1]).astype(jnp.bfloat16)
                    value = jnp.where(block >= 0, value, jnp.zeros_like(value))
                    if folded:
                        outs[owner // folded][owner % folded, :, lanes] = value
                    else:
                        outs[0][owner, index, :, lanes] = value


def pick(slots, counts, folded, after, slot_count, owners, me, block_slot, scales, codes):
    rows, cols = codes.shape[1:]
    if folded:
        shapes = [jax.ShapeDtypeStruct((folded, rows, cols), jnp.bfloat16)] * (owners // folded)
    else:
        shapes = [jax.ShapeDtypeStruct((owners, len(slots), rows, cols), jnp.bfloat16)]
    return pl.pallas_call(
        functools.partial(pick_kernel, slots, slot_count, counts, folded, len(after)),
        out_shape=shapes,
        in_specs=[SMEM, SMEM, VMEM, HBM] + [HBM] * len(after),
        out_specs=[VMEM] * len(shapes),
        scratch_shapes=[
            pltpu.SMEM((owners * slot_count,), jnp.int32),
            pltpu.VMEM((len(slots), owners, rows, cols), jnp.bfloat16),
            pltpu.VMEM((owners * scales.shape[1], rows), jnp.float32),
            pltpu.SemaphoreType.DMA((len(slots), owners)),
        ],
        name="pick",
        cost_estimate=pl.CostEstimate(
            flops=len(slots) * 4000000000, bytes_accessed=4 * owners * rows * cols, transcendentals=0
        ),
    )(me, block_slot, scales, codes, *after)


def tile_of(owner, stripes, rows):
    return owner // stripes, pl.ds(owner % stripes * rows, rows)


def gradient_copies(received, position, me, grad, grad_panels, sems):
    rows, width = received[0].shape[-2:]
    stripes = grad.shape[0] // rows
    copies = []
    for index in range(stripes * (grad.shape[1] // width)):
        if position is None:
            source = received[index % stripes].at[index // stripes]
            column, stripe = (me[0] // stripes) ^ (index // stripes), (me[0] % stripes) ^ (
                index % stripes
            )
        else:
            source = received[0].at[index, position]
            column, stripe = index // stripes, index % stripes
        at = pl.ds(pl.multiple_of(stripe * rows, rows), rows)
        whole = grad.at[at, pl.ds(pl.multiple_of(column * width, width), width)]
        copies.append(pltpu.make_async_copy(source, whole, sems.at[0, index]))
        if grad_panels is not None:
            copies.append(
                pltpu.make_async_copy(source, grad_panels.at[column, at], sems.at[1, index])
            )
    return copies


def start_gradient(received, position, limit, me, grad, grad_panels, sems):
    def start():
        for copy in gradient_copies(received, position, me, grad, grad_panels, sems):
            copy.start()

    if limit is None:
        return start()
    pl.when(me[0] < limit)(start)

    @pl.when(me[0] >= limit)
    def _():
        grad[...] = jnp.zeros(grad.shape, jnp.bfloat16)
        if grad_panels is not None:
            grad_panels[...] = jnp.zeros(grad_panels.shape, jnp.bfloat16)


def wait_gradient(received, position, limit, me, grad, grad_panels, sems):
    def wait():
        for copy in gradient_copies(received, position, me, grad, grad_panels, sems):
            copy.wait()

    if limit is None:
        return wait()
    pl.when(me[0] < limit)(wait)


def chain_kernel(slot, limit, parts, place_in, sends, chained, me, *refs):
    received, refs = refs[:parts], refs[parts:]
    lefts, rights, firsts, seconds = refs[:4]
    refs = refs[4 + chained :]
    send_refs, refs = refs[: len(sends)], refs[len(sends) :]
    first_out, second_out = refs[:2]
    grad, left, left_panels, right, first, second, direction, back, sems, out_sems = refs[2:]
    panels, side, width = back.shape
    rows_of_tile = received[0].shape[-2]
    gradient = (received, place_in, limit, me, grad, None, sems)
    basis = [
        pltpu.make_async_copy(
            lefts.at[slot, :, pl.ds(index * width, width)],
            left_panels.at[index],
            out_sems.at[2, index],
        )
        for index in range(panels)
    ]
    rest = [
        pltpu.make_async_copy(source.at[slot], target, out_sems.at[0, index])
        for index, (source, target) in enumerate(
            ((rights, right), (firsts, first), (seconds, second), (lefts, left))
        )
    ]
    start_gradient(*gradient)
    for copy in basis + rest:
        copy.start()
    wait_gradient(*gradient)
    for copy in basis + rest[:3]:
        copy.wait()

    def rotate(index, carry):
        rows = pl.ds(pl.multiple_of(index * width, width), width)
        half = dot(left_panels[index].T, grad[...]).astype(jnp.bfloat16)
        rotated = dot(half, right[...])
        moment_one = beta_first * first[rows, :].astype(jnp.float32) + (1.0 - beta_first) * rotated
        moment_two = (
            beta_second * second[rows, :].astype(jnp.float32)
            + (1.0 - beta_second) * rotated * rotated
        )
        first[rows, :] = moment_one.astype(jnp.bfloat16)
        second[rows, :] = moment_two.astype(jnp.bfloat16)
        direction[rows, :] = (moment_one / (jnp.sqrt(moment_two) + epsilon)).astype(jnp.bfloat16)
        return carry

    lax.fori_loop(0, panels, rotate, 0)
    moments_out = [
        pltpu.make_async_copy(first, first_out.at[slot], out_sems.at[1, 0]),
        pltpu.make_async_copy(second, second_out.at[slot], out_sems.at[1, 1]),
    ]
    for copy in moments_out:
        copy.start()
    rest[3].wait()

    def rotate_back(index, carry):
        rows = pl.ds(pl.multiple_of(index * width, width), width)
        half_back = dot(left[rows, :], direction[...]).astype(jnp.bfloat16)
        whole = dot(half_back, right[...], 1, 1).astype(jnp.bfloat16)
        for column in range(panels):
            back[column, rows, :] = whole[:, column * width : (column + 1) * width]
        return carry

    lax.fori_loop(0, panels, rotate_back, 0)
    sends_out = []
    for index, ranges in enumerate(sends):
        for low, high, position in ranges:
            for owner in range(low, high):
                column, rows = tile_of(owner, side // rows_of_tile, rows_of_tile)
                if isinstance(position, tuple):
                    length, depth = position
                    at = me[0] ^ owner
                    target = send_refs[index].at[at % length, at // length % depth]
                else:
                    target = send_refs[index].at[owner, position]
                sends_out.append(
                    pltpu.make_async_copy(back.at[column, rows], target, sems.at[0, owner])
                )

    def send(method):
        def act():
            for copy in sends_out:
                getattr(copy, method)()

        if limit is None:
            act()
        else:
            pl.when(me[0] < limit)(act)

    send("start")
    for copy in moments_out:
        copy.wait()
    send("wait")


def chain_step(slot, limit, place_in, sends, leads, targets, state, me, received, arrays):
    rows, width = received[0].shape[-2:]
    side = arrays[0].shape[1]
    panels = side // width
    owners = panels * (side // rows)
    square = pltpu.VMEM((side, side), jnp.bfloat16)
    columns = pltpu.VMEM((panels, side, width), jnp.bfloat16)
    aliased, aliases = [], {}
    for index, target in enumerate(list(targets) + list(state)):
        if target is not None:
            aliases[5 + len(received) + len(aliased)] = index
            aliased.append(target)
    moved = [
        jax.ShapeDtypeStruct(lead + (rows, width), jnp.bfloat16) for lead in leads
    ]
    kept = jax.ShapeDtypeStruct(arrays[0].shape, jnp.bfloat16)
    results = pl.pallas_call(
        functools.partial(
            chain_kernel, slot, limit, len(received), place_in, sends, len(aliased)
        ),
        out_shape=moved + [kept] * 2,
        in_specs=[SMEM] + [HBM] * (4 + len(received) + len(aliased)),
        out_specs=[HBM] * (len(sends) + 2),
        scratch_shapes=[
            square,
            square,
            columns,
            square,
            square,
            square,
            square,
            columns,
            pltpu.SemaphoreType.DMA((1, owners)),
            pltpu.SemaphoreType.DMA((3, max(4, panels))),
        ],
        input_output_aliases=aliases,
        name="chain",
        cost_estimate=pl.CostEstimate(
            flops=8 * side**3, bytes_accessed=16 * side * side, transcendentals=side * side
        ),
    )(me, *received, *arrays[:4], *aliased)
    return results[: len(sends)], results[len(sends) :]


def gram_kernel(slot, limit, parts, place_in, extra, me, *refs):
    received, (left_grams, right_grams), refs = refs[:parts], refs[parts : parts + 2], refs[parts + 2 :]
    left_out, right_out, grad, grad_panels, left_gram, right_gram, sems, out_sems = refs[extra:]
    panels, _, width = grad_panels.shape
    gradient = (received, place_in, limit, me, grad, grad_panels, sems)
    loads = [
        pltpu.make_async_copy(left_grams.at[slot], left_gram, out_sems.at[0]),
        pltpu.make_async_copy(right_grams.at[slot], right_gram, out_sems.at[1]),
    ]
    start_gradient(*gradient)
    for copy in loads:
        copy.start()
    wait_gradient(*gradient)
    for copy in loads:
        copy.wait()

    def grams(index, carry):
        rows = pl.ds(pl.multiple_of(index * width, width), width)
        left_new = gram_decay * left_gram[rows, :].astype(jnp.float32) + (
            1.0 - gram_decay
        ) * dot(grad[rows, :], grad[...], 1, 1)
        left_gram[rows, :] = left_new.astype(jnp.bfloat16)
        right_new = gram_decay * right_gram[rows, :].astype(jnp.float32) + (
            1.0 - gram_decay
        ) * dot(grad_panels[index].T, grad[...])
        right_gram[rows, :] = right_new.astype(jnp.bfloat16)
        return carry

    lax.fori_loop(0, panels, grams, 0)
    stores = [
        pltpu.make_async_copy(left_gram, left_out.at[slot], out_sems.at[0]),
        pltpu.make_async_copy(right_gram, right_out.at[slot], out_sems.at[1]),
    ]
    for copy in stores:
        copy.start()
    for copy in stores:
        copy.wait()


def gram_step(slot, limit, place_in, state, after, me, received, arrays):
    rows, width = received[0].shape[-2:]
    side = arrays[0].shape[1]
    panels = side // width
    owners = panels * (side // rows)
    square = pltpu.VMEM((side, side), jnp.bfloat16)
    aliased = [array for array in state if array is not None]
    kept = jax.ShapeDtypeStruct(arrays[0].shape, jnp.bfloat16)
    extra = len(aliased) + len(after)
    return pl.pallas_call(
        functools.partial(gram_kernel, slot, limit, len(received), place_in, extra),
        out_shape=[kept] * 2,
        in_specs=[SMEM] + [HBM] * (2 + len(received) + extra),
        out_specs=[HBM] * 2,
        scratch_shapes=[
            square,
            pltpu.VMEM((panels, side, width), jnp.bfloat16),
            square,
            square,
            pltpu.SemaphoreType.DMA((2, owners)),
            pltpu.SemaphoreType.DMA((2,)),
        ],
        input_output_aliases={
            3 + len(received) + index: index for index in range(len(aliased))
        },
        name="gram",
        cost_estimate=pl.CostEstimate(
            flops=4 * side**3, bytes_accessed=12 * side * side, transcendentals=0
        ),
    )(me, *received, *arrays[4:], *aliased, *after)


def place_kernel(jobs, slot_count, total, chained, me, block_slot, *refs):
    sources = refs[:total]
    out, holder, tiles, sems, out_sems = refs[total + chained :]
    fill_holder(block_slot, holder)

    def each(stage):
        start = 0
        for source, position, slot, count, low, high, order in jobs:

            def move(here, owner, taken, slot=slot):
                block = holder[owner * slot_count + slot]

                def arrive():
                    return pltpu.make_async_copy(taken, tiles.at[here], sems.at[here])

                def leave():
                    return pltpu.make_async_copy(tiles.at[here], out.at[block], out_sems.at[here])

                @pl.when(block >= 0)
                def _():
                    if stage == 0:
                        arrive().start()
                    elif stage == 1:
                        arrive().wait()
                        leave().start()
                    else:
                        leave().wait()

            def act(index, carry, source=source, position=position, move=move, start=start):
                move(start + index, index, sources[source].at[index, position])
                return carry

            @pl.when(jnp.logical_and(me[0] >= low, me[0] < high))
            def _():
                if order is None:
                    lax.fori_loop(0, count, act, 0)
                else:
                    first, spread = order
                    for index in range(count):
                        if spread:
                            taken = sources[source + index].at[position]
                        else:
                            taken = sources[source].at[index, position]
                        move(start + index, me[0] ^ (first + index), taken)

            start += count

    for stage in range(3):
        each(stage)


def place(jobs, slot_count, owners, update, shape, me, block_slot, sources):
    chained = 0 if update is None else 1
    total = sum(job[3] for job in jobs)
    return pl.pallas_call(
        functools.partial(place_kernel, jobs, slot_count, len(sources), chained),
        out_shape=jax.ShapeDtypeStruct(shape, jnp.bfloat16),
        in_specs=[SMEM, SMEM] + [HBM] * (len(sources) + chained),
        out_specs=HBM,
        scratch_shapes=[
            pltpu.SMEM((owners * slot_count,), jnp.int32),
            pltpu.VMEM((total,) + shape[1:], jnp.bfloat16),
            pltpu.SemaphoreType.DMA((total,)),
            pltpu.SemaphoreType.DMA((total,)),
        ],
        input_output_aliases={2 + len(sources): 0} if chained else {},
        name="place",
        cost_estimate=pl.CostEstimate(
            flops=1000000000,
            bytes_accessed=4 * total * shape[1] * shape[2],
            transcendentals=0,
        ),
    )(me, block_slot, *sources, *([update] if chained else []))


def regroup_kernel(positions, limit, count, *refs):
    refs, (outs, sems) = refs[: -len(positions) - 1], (refs[-len(positions) - 1 : -1], refs[-1])

    def gather(sources, first):
        copies = []
        for position, out in zip(positions, outs):
            for index, source in enumerate(sources):
                copies.append(
                    pltpu.make_async_copy(
                        source.at[position - first], out.at[index, 0], sems.at[len(copies)]
                    )
                )
        for copy in copies:
            copy.start()
        for copy in copies:
            copy.wait()

    if limit is None:
        gather(refs, 0)
    else:
        me = refs[0]
        pl.when(me[0] < limit)(lambda: gather(refs[1 : 1 + count], 0))
        pl.when(me[0] >= limit)(lambda: gather(refs[1 + count :], positions[0]))


def regroup(positions, arrays, limit=None, me=None, others=()):
    rows, width = arrays[0].shape[1:]
    total = len(positions) * len(arrays)
    scalars = () if limit is None else (me,)
    return pl.pallas_call(
        functools.partial(regroup_kernel, positions, limit, len(arrays)),
        out_shape=[
            jax.ShapeDtypeStruct((len(arrays), 1, rows, width), jnp.bfloat16) for _ in positions
        ],
        in_specs=[SMEM] * len(scalars) + [HBM] * (len(arrays) + len(others)),
        out_specs=[VMEM] * len(positions),
        scratch_shapes=[pltpu.SemaphoreType.DMA((total,))],
        name="regroup",
        cost_estimate=pl.CostEstimate(
            flops=1000000000, bytes_accessed=4 * total * rows * width, transcendentals=0
        ),
    )(*scalars, *arrays, *others)


def exchange(tiles):
    return lax.all_to_all(tiles, AXES, split_axis=0, concat_axis=0, tiled=True)


def fold(arrays, dp_count, tensor_count):
    moved = [arrays[0]]
    for shift in range(1, dp_count):
        moved.append(
            lax.ppermute(arrays[shift], "dp", [(at, at ^ shift) for at in range(dp_count)])
        )
    given = []
    for shift in range(tensor_count):
        stacked = jnp.stack([array[shift] for array in moved])
        if shift:
            stacked = lax.ppermute(
                stacked, "tensor", [(at, at ^ shift) for at in range(tensor_count)]
            )
        given.append(stacked)
    return given


def on_device(grad_codes, grad_scales, block_slot, *arrays):
    dp_count = lax.axis_size("dp")
    tensor_count = lax.axis_size("tensor")
    owners = dp_count * tensor_count
    slot_count = arrays[0].shape[0]
    block_rows, tile_rows, block_cols, tile_cols = grad_codes.shape
    blocks = block_rows * block_cols
    me = (lax.axis_index("dp") * tensor_count + lax.axis_index("tensor")).astype(jnp.int32)
    me = me.reshape(1)
    codes = grad_codes.transpose(0, 2, 1, 3).reshape(blocks, tile_rows, tile_cols)
    scales = grad_scales.transpose(0, 2, 3, 1).reshape(blocks, -1, tile_rows)
    shape = (blocks, tile_rows, tile_cols)
    half = owners // 2
    merged = (
        slot_count > 2
        and blocks == owners * (slot_count - 1) + half
        and dp_count & (dp_count - 1) == 0
        and tensor_count & (tensor_count - 1) == 0
    )

    def take(slots, counts, folded=None, after=()):
        return pick(
            slots, counts, folded, after, slot_count, owners, me, block_slot, scales, codes
        )

    def chain(slot, received, place_in, state, sends, leads, targets, limit=None):
        return chain_step(
            slot, limit, place_in, sends, leads, targets, state, me, received, arrays
        )

    def gram(slot, received, place_in, state, after, limit=None):
        return gram_step(slot, limit, place_in, state, after, me, received, arrays)

    def put(jobs, update, sources):
        return place(tuple(jobs), slot_count, owners, update, shape, me, block_slot, sources)

    moments, grams, update = (None, None), (None, None), None
    if not merged:
        received = [exchange(take((slot,), (owners,))[0]) for slot in range(slot_count)]
        for slot in range(slot_count):
            (sent,), moments = chain(
                slot, received[slot : slot + 1], 0, moments, (((0, owners, 0),),), ((owners, 1),), (None,)
            )
            grams = gram(slot, received[slot : slot + 1], 0, grams, ())
            update = put([(0, 0, slot, owners, 0, owners, None)], update, (exchange(sent),))
    else:
        last = slot_count - 1
        middle = tuple(range(1, last))
        first = take((0,), (owners,), tensor_count)
        bulk = take(middle, (owners,) * len(middle), None, first[-1:])[0]
        bulk = exchange(bulk)
        first = fold(first, dp_count, tensor_count)
        early = take((last,), (half,))[0]
        depth = dp_count // 2
        (early, slow), moments = chain(
            0,
            first,
            None,
            moments,
            (((half, owners, 0),), ((0, half, (tensor_count, depth)),)),
            ((owners, 1), (tensor_count, depth)),
            (early, None),
        )

        def along_tensor(array):
            moved = [array[0]]
            for shift in range(1, tensor_count):
                ring = [(at, at ^ shift) for at in range(tensor_count)]
                moved.append(lax.ppermute(array[shift], "tensor", ring))
            return moved

        def along_dp(pieces, shifts, count):
            return {
                shift: lax.ppermute(piece, "dp", [(at, at ^ shift) for at in range(count)])
                for shift, piece in zip(shifts, pieces)
            }

        across, beside = range(depth, dp_count), range(1, depth)
        slow = along_tensor(slow)
        early = exchange(early)
        slow_beside = along_dp(regroup(beside, slow), beside, depth)
        sent = None
        for index, slot in enumerate(middle):
            (sent,), moments = chain(
                slot,
                [bulk],
                index,
                moments,
                (((0, owners, index),),),
                ((owners, len(middle)),),
                (sent,),
            )
        returned = exchange(sent)
        (late,), moments = chain(
            last,
            [early],
            0,
            moments,
            (((0, owners, (tensor_count, dp_count)),),),
            ((tensor_count, dp_count),),
            (None,),
            half,
        )
        late = along_tensor(late)
        far = along_dp(regroup(across, late, half, me, slow), across, dp_count)
        late_beside = along_dp(regroup(beside, late), beside, depth)
        grams = gram(0, first, None, grams, (early,))
        for index, slot in enumerate(middle):
            grams = gram(slot, [bulk], index, grams, ())
        grams = gram(last, [early], 0, grams, (), half)
        jobs = [(0, index, slot, owners, 0, owners, None) for index, slot in enumerate(middle)]
        jobs.append((1, 0, 0, owners, half, owners, None))
        sources = [returned, early, *slow, *late]
        jobs.append((2, 0, 0, tensor_count, 0, half, (0, True)))
        jobs.append((2 + tensor_count, 0, last, tensor_count, 0, half, (0, True)))
        for shift, array in slow_beside.items():
            order = (shift * tensor_count, False)
            jobs.append((len(sources), 0, 0, tensor_count, 0, half, order))
            sources.append(array)
        update = put(jobs, update, sources)
        jobs, sources = [], []
        for shift, array in (*far.items(), *late_beside.items()):
            order = (shift * tensor_count, False)
            if shift in across:
                jobs.append((len(sources), 0, 0, tensor_count, 0, half, order))
                jobs.append((len(sources), 0, last, tensor_count, half, owners, order))
            else:
                jobs.append((len(sources), 0, last, tensor_count, 0, half, order))
            sources.append(array)
        update = put(jobs, update, sources)
    state = (*moments, *grams)
    update = update.reshape(block_rows, block_cols, tile_rows, tile_cols).transpose(0, 2, 1, 3)
    return (update, *state)


def solution(mesh):
    tiled = P(None, "tensor", None, "dp")
    owned = P(AXES, None, None)

    return jax.shard_map(
        on_device,
        mesh=mesh,
        in_specs=(tiled, tiled, P()) + (owned,) * 6,
        out_specs=(tiled,) + (owned,) * 4,
        check_vma=False,
    )
```
